32 devices in a mesh: rows: 8 (over z, x), tp: 2 (over core), job: 2 (over y).
Axes of the slice: x: 2, y: 2, z: 4, core: 2. Of those that a mesh axis runs over, the one named last changes fastest.
Arguments:
- train_query: bfloat16 [4096, 2048], P(('job', 'rows'), 'tp'), parts along dimension 0, may hold values from -0.125 to 0.125
- low_query: bfloat16 [4096, 16], P(('job', 'rows')), parts along dimension 0, may hold values from -0.125 to 0.125
- high_query: bfloat16 [32, 2048], P('job', 'tp'), parts along dimension 0, may hold values from -1.5 to 1.5
- train_key: bfloat16 [4096, 512], P(('job', 'rows'), 'tp'), parts along dimension 0, may hold values from -0.125 to 0.125
- low_key: bfloat16 [4096, 16], P(('job', 'rows')), parts along dimension 0, may hold values from -0.125 to 0.125
- high_key: bfloat16 [32, 512], P('job', 'tp'), parts along dimension 0, may hold values from -1.5 to 1.5
- train_value: bfloat16 [4096, 512], P(('job', 'rows'), 'tp'), parts along dimension 0, may hold values from -0.125 to 0.125
- low_value: bfloat16 [4096, 16], P(('job', 'rows')), parts along dimension 0, may hold values from -0.125 to 0.125
- high_value: bfloat16 [32, 512], P('job', 'tp'), parts along dimension 0, may hold values from -1.5 to 1.5
- norm_train: float32 [4096], P(('job', 'rows', 'tp')), parts along dimension 0, may hold values from 0.25 to 1.75
- norm_step: float32 [4096], P(('job', 'rows', 'tp')), parts along dimension 0, may hold values from -0.3 to 0.3
Outputs:
- serve_query: bfloat16 [4096, 2048], P(('job', 'tp')), parts along dimension 0
- serve_key: bfloat16 [1024, 2048], P(('job', 'tp')), parts along dimension 0
- serve_value: bfloat16 [1024, 2048], P(('job', 'tp')), parts along dimension 0
- serve_norm: bfloat16 [4096], P('job'), parts along dimension 0
The draws below stay inside these ranges and needn't reach their ends.
There are 2 independent parts, one for each index of `job`. The reference program is written for one: setup_inputs(seed, part) draws one part's arguments, and reference() takes and returns one part's arrays. A program takes and returns all parts, laid end to end along the dimension named above; each array names one. Nothing has to cross between parts.
All inputs are finite; a program needn't handle non-finite values.
Results may differ from the reference program's by a relative error of at most 0.001.
Values may be sent and summed in bfloat16 or wider, within the bound.
A program may use at most 64 MiB of HBM per device.

```python
import jax
import jax.numpy as jnp

D_MODEL = 2048
Q_DIM = 2048
KV_DIM = 512
RANK = 16


def level_of(stream_key, extent, pieces, low, top_value):
    gain = 1.0
    for dim, blocks in pieces:
        heights = jax.random.uniform(jax.random.fold_in(jax.random.fold_in(stream_key, 6), dim), (blocks,), jnp.float32, low / len(pieces), top_value / len(pieces))
        gain = gain * jnp.repeat(jnp.exp(heights), extent[dim] // blocks).reshape((-1,) + (1,) * (len(extent) - 1 - dim))
    return gain


def centred(own_key, shape, spread, reach, cuts=(), kind=jnp.bfloat16):
    entries = spread * jax.random.normal(own_key, shape, jnp.float32)
    if cuts:
        entries = entries * level_of(own_key, shape, cuts, -0.22, 0.18)
    return jnp.clip(entries, -reach, reach).astype(kind)


def setup_inputs(seed: int = 0, part: int = 0) -> dict:
    key_of = jax.random.split(jax.random.key(seed), 12)
    own_keys = jax.random.split(jax.random.fold_in(key_of[11], part), 12)
    return {
        "train_query": centred(own_keys[0], (D_MODEL, Q_DIM), D_MODEL ** -0.5, 0.125, ((0, 8), (1, 2))),
        "low_query": centred(own_keys[1], (D_MODEL, RANK), D_MODEL ** -0.5, 0.125, ((0, 8),)),
        "high_query": centred(own_keys[2], (RANK, Q_DIM), RANK ** -0.5, 1.5, ((1, 2),)),
        "train_key": centred(own_keys[3], (D_MODEL, KV_DIM), D_MODEL ** -0.5, 0.125, ((0, 8), (1, 2))),
        "low_key": centred(own_keys[4], (D_MODEL, RANK), D_MODEL ** -0.5, 0.125, ((0, 8),)),
        "high_key": centred(own_keys[5], (RANK, KV_DIM), RANK ** -0.5, 1.5, ((1, 2),)),
        "train_value": centred(own_keys[6], (D_MODEL, KV_DIM), D_MODEL ** -0.5, 0.125, ((0, 8), (1, 2))),
        "low_value": centred(own_keys[7], (D_MODEL, RANK), D_MODEL ** -0.5, 0.125, ((0, 8),)),
        "high_value": centred(own_keys[8], (RANK, KV_DIM), RANK ** -0.5, 1.5, ((1, 2),)),
        "norm_train": jnp.clip(1.0 + 0.15 * jax.random.normal(own_keys[9], (D_MODEL,), jnp.float32), 0.25, 1.75),
        "norm_step": jnp.clip(jax.random.uniform(own_keys[10], (D_MODEL,), jnp.float32, -0.3, 0.3) * level_of(own_keys[10], (D_MODEL,), ((0, 16),), -0.4, 0.0), -0.3, 0.3),
    }


mix_rate = 0.5


def reference(train_query, low_query, high_query, train_key, low_key, high_key, train_value, low_value, high_value, norm_train, norm_step):
    fresh_query = train_query.astype(jnp.float32) + mix_rate * jnp.dot(low_query, high_query, preferred_element_type=jnp.float32)
    fresh_key = train_key.astype(jnp.float32) + mix_rate * jnp.dot(low_key, high_key, preferred_element_type=jnp.float32)
    fresh_value = train_value.astype(jnp.float32) + mix_rate * jnp.dot(low_value, high_value, preferred_element_type=jnp.float32)
    serve_query = fresh_query.T.astype(jnp.bfloat16)
    serve_key = fresh_key.T.astype(jnp.bfloat16)
    serve_value = fresh_value.T.astype(jnp.bfloat16)
    serve_norm = (norm_train + norm_step).astype(jnp.bfloat16)
    return serve_query, serve_key, serve_value, serve_norm
```

```python
import functools

import jax
import jax.numpy as jnp
from jax import lax
from jax.experimental import pallas as pl
from jax.experimental.pallas import tpu as pltpu
from jax.sharding import PartitionSpec as P

mix_rate = 0.5
CHUNK_ROWS = 256
FIRST_ROWS = 256
VMEM_BYTES = 67043328
MESH = pl.DeviceIdType.MESH


def cuts(length, first):
    sizes = []
    while first and length > FIRST_ROWS and length % (2 * FIRST_ROWS) == 0:
        sizes.insert(0, min(length // 2, CHUNK_ROWS))
        length -= sizes[0]
    while length:
        sizes.insert(0, min(length, FIRST_ROWS if first else CHUNK_ROWS))
        length -= sizes[0]
    start, found = 0, []
    for rows in sizes:
        found.append((start, rows))
        start += rows
    return found


def kernel(
    size,
    tp_size,
    *refs,
):
    given, refs = refs[:11], refs[11:]
    serve_query, serve_key, serve_value, serve_norm = refs[:4]
    held, refs = refs[4:15], refs[15:]
    run_kernel(size, tp_size, given, held, serve_query, serve_key, serve_value, serve_norm, *refs)


def run_kernel(
    size,
    tp_size,
    given,
    held,
    serve_query,
    serve_key,
    serve_value,
    serve_norm,
    gains,
    load_sem,
    send_sem,
    line_sem,
    cross_sem,
    rest_sem,
    gain_send,
    gain_line,
    gain_rest,
    pair_send,
    pair_recv,
):
    loads = [
        pltpu.make_async_copy(g, h, load_sem.at[n]) for n, (g, h) in enumerate(zip(given, held))
    ]
    (
        train_query,
        low_query,
        high_query,
        train_key,
        low_key,
        high_key,
        train_value,
        low_value,
        high_value,
        norm_train,
        norm_step,
    ) = held
    depth = size // 2
    me = lax.axis_index("rows")
    core = lax.axis_index("tp")
    z, x = me // 2, lax.rem(me, 2)
    other = 1 - x
    width = train_query.shape[0]
    up, down, side = me + 2, me - 2, 2 * z + other
    targets = (up, down, side)
    has_up, has_down = z < depth - 1, z > 0
    UP, DOWN, SIDE = 0, 1, 2

    def partner(k):
        return {"tp": lax.rem(core + k, tp_size)}

    barrier = pltpu.get_barrier_semaphore()

    def greet(device):
        pl.semaphore_signal(barrier, inc=1, device_id=device, device_id_type=MESH)

    @pl.when(has_up)
    def _():
        greet({"rows": up})

    @pl.when(has_down)
    def _():
        greet({"rows": down})

    greet({"rows": side})
    for k in range(1, tp_size):
        greet(partner(k))
    for load in loads:
        load.start()

    chunks = []
    for train, low, high, serve in (
        (train_query, low_query, high_query, serve_query),
        (train_key, low_key, high_key, serve_key),
        (train_value, low_value, high_value, serve_value),
    ):
        for start, rows in cuts(serve.shape[0], not chunks):
            chunks.append((train, low, high, serve, start, rows))
    count = len(chunks)
    queries = sum(c[3] is serve_query for c in chunks)
    twice, left = set(), sum(c[5] for c in chunks) // 2
    for c in sorted(range(count), key=lambda c: -chunks[c][5]):
        if chunks[c][5] <= left:
            twice.add(c)
            left -= chunks[c][5]

    crossings = sorted(twice)
    tall = sum(c[5] for c in chunks)
    cross_tall = sum(chunks[c][5] for c in crossings)

    def piece(item, c):
        if c == count:
            return gains.at[item]
        serve, start, rows = chunks[c][3:]
        return serve.at[pl.ds(start, rows), pl.ds(pl.multiple_of(item * width, 128), width)]

    def landing(item, c, way, own_side):
        if c == count:
            return gain_rest.at[0] if way == SIDE else gain_line.at[item // 2]
        if way != SIDE:
            return line_sem.at[item // 2, c]
        if own_side and crossing(c):
            return cross_sem.at[crossings.index(c)]
        return rest_sem.at[0]

    def copy(item, c, way, recv):
        ref = piece(item, c)
        return pltpu.make_async_remote_copy(
            src_ref=ref,
            dst_ref=ref,
            send_sem=gain_send.at[way] if c == count else send_sem.at[way],
            recv_sem=recv,
            device_id={"rows": targets[way]},
            device_id_type=MESH,
        )

    def send(item, c, way, own=False):
        copy(item, c, way, landing(item, c, way, own)).start()

    def arrive_line(item, c):
        copy(item, c, UP, landing(item, c, UP, False)).wait_recv()

    def bulk(ref, send, recv):
        return pltpu.make_async_remote_copy(
            src_ref=ref,
            dst_ref=ref,
            send_sem=send,
            recv_sem=recv,
            device_id={"rows": side},
            device_id_type=MESH,
        )

    def span(rows):
        return serve_query.at[pl.ds(0, rows // size), :]

    def crossing(c):
        return c in twice

    def merge(c):
        train, low, high, serve, start, length = chunks[c]
        rows = pl.ds(start, length)
        update = lax.dot_general(
            high[:, rows], low[...], (((0,), (0,)), ((), ())), preferred_element_type=jnp.float32
        )
        fresh = train[:, rows].T.astype(jnp.float32) + mix_rate * update
        serve[rows, pl.ds(pl.multiple_of(me * width, 128), width)] = fresh.astype(jnp.bfloat16)

    def send_own(c):
        @pl.when(has_down)
        def _():
            send(me, c, DOWN)

        @pl.when(has_up)
        def _():
            send(me, c, UP)

        send(me, c, SIDE, own=True)

    def gain_copy(k):
        return pltpu.make_async_remote_copy(
            src_ref=gains.at[me, core],
            dst_ref=gains.at[me, core],
            send_sem=pair_send.at[k],
            recv_sem=pair_recv.at[k],
            device_id=partner(k),
            device_id_type=MESH,
        )

    for n in (0, 1, 2, 9, 10):
        loads[n].wait()
    gains[pl.ds(me, 1), pl.ds(core, 1)] = (norm_train[...] + norm_step[...])[None, None]
    merge(0)
    merge(1)
    pl.semaphore_wait(barrier, tp_size + has_up.astype(jnp.int32) + has_down.astype(jnp.int32))
    for c in range(2, count + 2):
        send_own(c - 2)
        if c < count:
            if c == queries:
                for n in range(3, 9):
                    loads[n].wait()
            merge(c)
        if c == 3:
            for k in range(1, tp_size):
                gain_copy(k).start()
    for k in range(1, tp_size):
        gain_copy(k).wait_recv()
    send_own(count)

    def pass_on(step, c):
        below, above = me - 2 * step, me + 2 * step

        @pl.when(z >= step)
        def _():
            arrive_line(below, c)

            @pl.when(has_up)
            def _():
                send(below, c, UP)

            if not (step == 1 and crossing(c)):
                send(below, c, SIDE)

        @pl.when(z + step < depth)
        def _():
            arrive_line(above, c)

            @pl.when(has_down)
            def _():
                send(above, c, DOWN)

            if not (step == 1 and crossing(c)):
                send(above, c, SIDE)

    def cross(c):
        copy(side, c, SIDE, landing(side, c, SIDE, True)).wait_recv()

        @pl.when(has_down)
        def _():
            copy(side, c, DOWN, rest_sem.at[0]).start()

        @pl.when(has_up)
        def _():
            copy(side, c, UP, rest_sem.at[0]).start()

    for step in range(1, depth):
        for c in range(count + 1):
            pass_on(step, c)
        if step == max(1, depth - 2):
            for c in crossings:
                cross(c)

    bulk(gains.at[pl.ds(0, depth)], gain_send.at[SIDE], gain_rest.at[0]).wait()
    serve_norm[...] = gains[...].reshape(serve_norm.shape).astype(jnp.bfloat16)
    bulk(span(depth * tall - cross_tall), send_sem.at[SIDE], rest_sem.at[0]).wait_recv()

    for k in range(1, tp_size):
        gain_copy(k).wait_send()
    for level in range(depth):
        up_rows = ((level + 1) * tall + cross_tall) if level < depth - 1 else 0
        down_rows = ((depth - level) * tall + cross_tall) if level else 0
        ends = (level > 0) + (level < depth - 1)

        @pl.when(z == level)
        def _():
            bulk(span(depth * tall - ends * cross_tall), send_sem.at[SIDE], rest_sem.at[0]).wait_send()
            for way, rows, items in (
                (UP, up_rows, level + 1),
                (DOWN, down_rows, depth - level),
            ):
                if rows:
                    bulk(span(rows), send_sem.at[way], rest_sem.at[0]).wait_send()
                    bulk(
                        gains.at[pl.ds(0, items)], gain_send.at[way], gain_rest.at[0]
                    ).wait_send()


def fused(size, tp_size, *args):
    train_query, train_key, train_value, norm_train = args[0], args[3], args[6], args[9]
    seats, norm_length = size * tp_size, norm_train.shape[0]
    args = [a.T if n in (1, 4, 7) else a for n, a in enumerate(args)]
    args = [a.reshape(1, -1) if a.ndim == 1 else a for a in args]
    full = train_query.shape[0] * size
    outs = [
        pltpu.VMEM((t.shape[1], full), jnp.bfloat16)
        for t in (train_query, train_key, train_value)
    ]
    outs.append(pltpu.VMEM((seats, norm_length), jnp.bfloat16))
    lengths = [t.shape[1] for t in (train_query, train_key, train_value)]
    count = sum(len(cuts(length, n == 0)) for n, length in enumerate(lengths))
    grant = VMEM_BYTES - 2 * (sum(t.shape[1] for t in (train_query, train_key, train_value)) * full)
    grant -= 2 * seats * norm_length
    vmem = pl.BlockSpec(memory_space=pltpu.VMEM)
    query, key, value, norm = pl.pallas_call(
        functools.partial(kernel, size, tp_size),
        out_shape=outs,
        in_specs=[pl.BlockSpec(memory_space=pltpu.HBM)] * 11,
        out_specs=[vmem] * 4,
        scratch_shapes=[pltpu.VMEM(a.shape, a.dtype) for a in args]
        + [
            pltpu.VMEM((size, tp_size, 1, norm_length), jnp.float32),
            pltpu.SemaphoreType.DMA((11,)),
            pltpu.SemaphoreType.DMA((3,)),
            pltpu.SemaphoreType.DMA((size // 2, count)),
            pltpu.SemaphoreType.DMA((count,)),
            pltpu.SemaphoreType.DMA((1,)),
            pltpu.SemaphoreType.DMA((3,)),
            pltpu.SemaphoreType.DMA((size // 2,)),
            pltpu.SemaphoreType.DMA((1,)),
            pltpu.SemaphoreType.DMA((tp_size,)),
            pltpu.SemaphoreType.DMA((tp_size,)),
        ],
        compiler_params=pltpu.CompilerParams(
            collective_id=0, has_side_effects=True, vmem_limit_bytes=grant
        ),
    )(*args)
    query, key, value, norm = store_out(query, key, value, norm)
    return query, key, value, norm.reshape(-1)


def store_kernel(*refs):
    ins, outs, sems = refs[:4], refs[4:8], refs[8]
    copies = [pltpu.make_async_copy(i, o, sems.at[n]) for n, (i, o) in enumerate(zip(ins, outs))]
    for c in copies:
        c.start()
    for c in copies:
        c.wait()


def store_out(*arrays):
    return pl.pallas_call(
        store_kernel,
        out_shape=[jax.ShapeDtypeStruct(a.shape, a.dtype) for a in arrays],
        in_specs=[pl.BlockSpec(memory_space=pltpu.VMEM)] * 4,
        out_specs=[pl.BlockSpec(memory_space=pltpu.HBM)] * 4,
        scratch_shapes=[pltpu.SemaphoreType.DMA((4,))],
        compiler_params=pltpu.CompilerParams(vmem_limit_bytes=16 * 2**20),
    )(*arrays)


def plain(
    train_query,
    low_query,
    high_query,
    train_key,
    low_key,
    high_key,
    train_value,
    low_value,
    high_value,
    norm_train,
    norm_step,
):
    def merged(train, low, high):
        update = jnp.dot(low, high, preferred_element_type=jnp.float32)
        fresh = train.astype(jnp.float32) + mix_rate * update
        return lax.all_gather(fresh.astype(jnp.bfloat16), "rows", axis=0, tiled=True).T

    serve_norm = lax.all_gather(
        (norm_train + norm_step).astype(jnp.bfloat16), ("rows", "tp"), axis=0, tiled=True
    )
    return (
        merged(train_query, low_query, high_query),
        merged(train_key, low_key, high_key),
        merged(train_value, low_value, high_value),
        serve_norm,
    )


def solution(mesh):
    size, tp_size = mesh.shape["rows"], mesh.shape["tp"]

    def local(*args):
        trains = (args[0], args[3], args[6])
        fits = (
            size % 2 == 0
            and size >= 4
            and all(t.shape[0] % 128 == 0 and t.shape[1] % FIRST_ROWS == 0 for t in trains)
            and args[9].shape[0] % 128 == 0
        )
        return fused(size, tp_size, *args) if fits else plain(*args)

    in_specs = (
        P(("job", "rows"), "tp"),
        P(("job", "rows"), None),
        P("job", "tp"),
        P(("job", "rows"), "tp"),
        P(("job", "rows"), None),
        P("job", "tp"),
        P(("job", "rows"), "tp"),
        P(("job", "rows"), None),
        P("job", "tp"),
        P(("job", "rows", "tp")),
        P(("job", "rows", "tp")),
    )
    out_specs = (P(("job", "tp"), None), P(("job", "tp"), None), P(("job", "tp"), None), P("job"))
    return jax.shard_map(local, mesh=mesh, in_specs=in_specs, out_specs=out_specs, check_vma=False)
```

```python
import functools

import jax
import jax.numpy as jnp
from jax import lax
from jax.experimental import pallas as pl
from jax.experimental.pallas import tpu as pltpu
from jax.sharding import PartitionSpec as P

mix_rate = 0.5
CHUNK_ROWS = 256
SMALL_ROWS = 128
RELIEF = 1
VMEM_BYTES = 67043328
MESH = pl.DeviceIdType.MESH


def cuts(length, first):
    sizes = [SMALL_ROWS] * 2 if first else []
    length -= sum(sizes)
    while length:
        sizes.append(min(length, CHUNK_ROWS))
        length -= sizes[-1]
    start, found = 0, []
    for rows in sizes:
        found.append((start, rows))
        start += rows
    return found


def crossed(rows):
    twice, left = [], sum(rows) // 2
    for c in sorted(range(len(rows)), key=lambda c: -rows[c]):
        if c != RELIEF and rows[c] <= left:
            twice.append(c)
            left -= rows[c]
    return sorted(twice)


def kernel(
    size,
    tp_size,
    *refs,
):
    given, refs = refs[:11], refs[11:]
    serve_query, serve_key, serve_value, serve_norm = refs[:4]
    held, refs = refs[4:15], refs[15:]
    run_kernel(size, tp_size, given, held, serve_query, serve_key, serve_value, serve_norm, *refs)


def run_kernel(
    size,
    tp_size,
    given,
    held,
    serve_query,
    serve_key,
    serve_value,
    serve_norm,
    gains,
    load_sem,
    send_sem,
    line_sem,
    cross_sem,
    rest_sem,
    gain_send,
    gain_line,
    gain_rest,
    pair_send,
    pair_recv,
    stage,
    stage_sem,
):
    loads = [
        pltpu.make_async_copy(g, h, load_sem.at[n]) for n, (g, h) in enumerate(zip(given, held))
    ]
    (
        train_query,
        low_query,
        high_query,
        train_key,
        low_key,
        high_key,
        train_value,
        low_value,
        high_value,
        norm_train,
        norm_step,
    ) = held
    depth = size // 2
    me = lax.axis_index("rows")
    core = lax.axis_index("tp")
    z, x = me // 2, lax.rem(me, 2)
    other = 1 - x
    width = train_query.shape[0]
    up, down, side = me + 2, me - 2, 2 * z + other
    targets = (up, down, side)
    has_up, has_down = z < depth - 1, z > 0
    UP, DOWN, SIDE = 0, 1, 2

    def partner(k):
        return {"tp": lax.rem(core + k, tp_size)}

    barrier = pltpu.get_barrier_semaphore()

    def greet(device):
        pl.semaphore_signal(barrier, inc=1, device_id=device, device_id_type=MESH)

    @pl.when(has_up)
    def _():
        greet({"rows": up})

    @pl.when(has_down)
    def _():
        greet({"rows": down})

    greet({"rows": side})
    for k in range(1, tp_size):
        greet(partner(k))
    job = lax.axis_index("job")
    near = (core == 0) & ((me == 1) | (me == 2))
    source, helper = near & (job == 0), near & (job == 1)

    @pl.when((core == 0) & (me == 0) & (job == 0))
    def _():
        for row in (1, 2):
            greet({"job": 1, "rows": row})

    @pl.when(helper)
    def _():
        greet({"job": 0})

    for load in loads:
        load.start()

    chunks = []
    for train, low, high, serve in (
        (train_query, low_query, high_query, serve_query),
        (train_key, low_key, high_key, serve_key),
        (train_value, low_value, high_value, serve_value),
    ):
        for start, rows in cuts(serve.shape[0], not chunks):
            chunks.append((train, low, high, serve, start, rows))
    count = len(chunks)
    queries = sum(c[3] is serve_query for c in chunks)
    crossings = crossed([c[5] for c in chunks])
    tall = sum(c[5] for c in chunks)
    cross_tall = sum(chunks[c][5] for c in crossings)

    def piece(item, c):
        if c == count:
            return gains.at[item]
        serve, start, rows = chunks[c][3:]
        return serve.at[pl.ds(start, rows), pl.ds(pl.multiple_of(item * width, 128), width)]

    def landing(item, c, way, own_side):
        if c == count:
            return gain_rest.at[0] if way == SIDE else gain_line.at[item // 2]
        if way != SIDE:
            return line_sem.at[item // 2, c]
        if own_side and crossing(c):
            return cross_sem.at[crossings.index(c)]
        return rest_sem.at[0]

    def copy(item, c, way, recv):
        ref = piece(item, c)
        return pltpu.make_async_remote_copy(
            src_ref=ref,
            dst_ref=ref,
            send_sem=gain_send.at[0] if c == count else send_sem.at[way],
            recv_sem=recv,
            device_id={"rows": targets[way]},
            device_id_type=MESH,
        )

    def send(item, c, way, own=False):
        copy(item, c, way, landing(item, c, way, own)).start()

    def arrive_line(item, c):
        copy(item, c, UP, landing(item, c, UP, False)).wait_recv()

    def bulk(ref, send, recv):
        return pltpu.make_async_remote_copy(
            src_ref=ref,
            dst_ref=ref,
            send_sem=send,
            recv_sem=recv,
            device_id={"rows": side},
            device_id_type=MESH,
        )

    def span(rows):
        return serve_query.at[pl.ds(0, rows // size), :]

    def crossing(c):
        return c in crossings

    def merge(c):
        train, low, high, serve, start, length = chunks[c]
        rows = pl.ds(start, length)
        update = lax.dot_general(
            high[:, rows], low[...], (((0,), (0,)), ((), ())), preferred_element_type=jnp.float32
        )
        fresh = train[:, rows].T.astype(jnp.float32) + mix_rate * update
        serve[rows, pl.ds(pl.multiple_of(me * width, 128), width)] = fresh.astype(jnp.bfloat16)

    def send_own(c):
        down, across = has_down, True
        if c == RELIEF:
            down, across = has_down & ~(source & (me == 2)), ~(source & (me == 1))

            @pl.when(source)
            def _():
                hand_over().start()

        @pl.when(down)
        def _():
            send(me, c, DOWN)

        @pl.when(has_up)
        def _():
            send(me, c, UP)

        @pl.when(across)
        def _():
            send(me, c, SIDE, own=True)

    def hand_over():
        return pltpu.make_async_remote_copy(
            src_ref=piece(me, RELIEF),
            dst_ref=stage,
            send_sem=stage_sem.at[0],
            recv_sem=stage_sem.at[1],
            device_id={"job": 1},
            device_id_type=MESH,
        )

    def relieve(way):
        return pltpu.make_async_remote_copy(
            src_ref=stage,
            dst_ref=piece(me, RELIEF),
            send_sem=stage_sem.at[2],
            recv_sem=landing(me, RELIEF, way, True),
            device_id={"job": 0, "rows": 0},
            device_id_type=MESH,
        )

    def gain_copy(k):
        return pltpu.make_async_remote_copy(
            src_ref=gains.at[me, core],
            dst_ref=gains.at[me, core],
            send_sem=pair_send.at[k - 1],
            recv_sem=pair_recv.at[k - 1],
            device_id=partner(k),
            device_id_type=MESH,
        )

    for n in (0, 1, 2, 9, 10):
        loads[n].wait()
    gains[pl.ds(me, 1), pl.ds(core, 1)] = (norm_train[...] + norm_step[...])[None, None]
    merge(0)
    merge(1)
    expected = sum(e.astype(jnp.int32) for e in (has_up, has_down, source, helper))
    pl.semaphore_wait(barrier, tp_size + expected)
    for c in range(2, count + 2):
        send_own(c - 2)
        if c < count:
            if c == queries:
                for n in range(3, 9):
                    loads[n].wait()
            merge(c)
        if c == 3:
            for k in range(1, tp_size):
                gain_copy(k).start()
    for k in range(1, tp_size):
        gain_copy(k).wait_recv()
    send_own(count)

    @pl.when(helper)
    def _():
        hand_over().wait_recv()

        @pl.when(me == 1)
        def _():
            relieve(SIDE).start()

        @pl.when(me == 2)
        def _():
            relieve(DOWN).start()

    def pass_on(step, c):
        below, above = me - 2 * step, me + 2 * step

        @pl.when(z >= step)
        def _():
            arrive_line(below, c)

            @pl.when(has_up)
            def _():
                send(below, c, UP)

            if not (step == 1 and crossing(c)):
                send(below, c, SIDE)

        @pl.when(z + step < depth)
        def _():
            arrive_line(above, c)

            @pl.when(has_down)
            def _():
                send(above, c, DOWN)

            if not (step == 1 and crossing(c)):
                send(above, c, SIDE)

    def cross(c):
        copy(side, c, SIDE, landing(side, c, SIDE, True)).wait_recv()

        @pl.when(has_down)
        def _():
            copy(side, c, DOWN, rest_sem.at[0]).start()

        @pl.when(has_up)
        def _():
            copy(side, c, UP, rest_sem.at[0]).start()

    order = [c for c in range(count + 1) if c != RELIEF] + [RELIEF]
    for step in range(1, depth):
        for c in order:
            pass_on(step, c)
        if step == max(1, depth - 2):
            for c in crossings:
                cross(c)

    bulk(gains.at[pl.ds(0, depth)], gain_send.at[0], gain_rest.at[0]).wait_recv()
    serve_norm[...] = gains[:size].reshape(serve_norm.shape).astype(jnp.bfloat16)
    bulk(span(depth * tall - cross_tall), send_sem.at[SIDE], rest_sem.at[0]).wait_recv()

    for k in range(1, tp_size):
        gain_copy(k).wait_send()
    @pl.when(source)
    def _():
        hand_over().wait_send()

    @pl.when(helper)
    def _():
        relieve(SIDE).wait_send()

    for level in range(depth):
        has = {UP: level < depth - 1, DOWN: level > 0, SIDE: True}
        rows = {
            UP: (level + 1) * tall + cross_tall,
            DOWN: (depth - level) * tall + cross_tall,
            SIDE: depth * tall - (has[UP] + has[DOWN]) * cross_tall,
        }
        items = {UP: level + 1, DOWN: depth - level, SIDE: depth}
        ways = [way for way in (UP, DOWN, SIDE) if has[way]]

        def drain(less):
            for way in ways:
                sent = span(rows[way] - less.get(way, 0))
                bulk(sent, send_sem.at[way], rest_sem.at[0]).wait_send()

        @pl.when((z == level) & ~source)
        def _():
            drain({})

        if level < 2:

            @pl.when((z == level) & source)
            def _():
                drain({DOWN if level else SIDE: chunks[RELIEF][5]})

        @pl.when(z == level)
        def _():
            sent = gains.at[pl.ds(0, sum(items[way] for way in ways))]
            bulk(sent, gain_send.at[0], gain_rest.at[0]).wait_send()


def fused(size, tp_size, *args):
    train_query, train_key, train_value, norm_train = args[0], args[3], args[6], args[9]
    seats, norm_length = size * tp_size, norm_train.shape[0]
    args = [a.T if n in (1, 4, 7) else a for n, a in enumerate(args)]
    args = [a.reshape(1, -1) if a.ndim == 1 else a for a in args]
    full = train_query.shape[0] * size
    outs = [
        pltpu.VMEM((t.shape[1], full), jnp.bfloat16)
        for t in (train_query, train_key, train_value)
    ]
    outs.append(pltpu.VMEM((seats, norm_length), jnp.bfloat16))
    lengths = [t.shape[1] for t in (train_query, train_key, train_value)]
    sizes = [rows for n, length in enumerate(lengths) for _, rows in cuts(length, n == 0)]
    count = len(sizes)
    grant = VMEM_BYTES - 2 * (sum(t.shape[1] for t in (train_query, train_key, train_value)) * full)
    grant -= 2 * seats * norm_length
    vmem = pl.BlockSpec(memory_space=pltpu.VMEM)
    query, key, value, norm = pl.pallas_call(
        functools.partial(kernel, size, tp_size),
        out_shape=outs,
        in_specs=[pl.BlockSpec(memory_space=pltpu.HBM)] * 11,
        out_specs=[vmem] * 4,
        scratch_shapes=[pltpu.VMEM(a.shape, a.dtype) for a in args]
        + [
            pltpu.VMEM((2 * size, tp_size, 1, norm_length), jnp.float32),
            pltpu.SemaphoreType.DMA((11,)),
            pltpu.SemaphoreType.DMA((3,)),
            pltpu.SemaphoreType.DMA((size // 2, count)),
            pltpu.SemaphoreType.DMA((len(crossed(sizes)),)),
            pltpu.SemaphoreType.DMA((1,)),
            pltpu.SemaphoreType.DMA((1,)),
            pltpu.SemaphoreType.DMA((size // 2,)),
            pltpu.SemaphoreType.DMA((1,)),
            pltpu.SemaphoreType.DMA((tp_size - 1,)),
            pltpu.SemaphoreType.DMA((tp_size - 1,)),
            pltpu.VMEM((SMALL_ROWS, train_query.shape[0]), jnp.bfloat16),
            pltpu.SemaphoreType.DMA((3,)),
        ],
        compiler_params=pltpu.CompilerParams(
            collective_id=0, has_side_effects=True, vmem_limit_bytes=grant
        ),
    )(*args)
    query, key, value, norm = store_out(query, key, value, norm)
    return query, key, value, norm.reshape(-1)


def store_kernel(*refs):
    ins, outs, sems = refs[:4], refs[4:8], refs[8]
    copies = [pltpu.make_async_copy(i, o, sems.at[n]) for n, (i, o) in enumerate(zip(ins, outs))]
    for c in copies:
        c.start()
    for c in copies:
        c.wait()


def store_out(*arrays):
    return pl.pallas_call(
        store_kernel,
        out_shape=[jax.ShapeDtypeStruct(a.shape, a.dtype) for a in arrays],
        in_specs=[pl.BlockSpec(memory_space=pltpu.VMEM)] * 4,
        out_specs=[pl.BlockSpec(memory_space=pltpu.HBM)] * 4,
        scratch_shapes=[pltpu.SemaphoreType.DMA((4,))],
        compiler_params=pltpu.CompilerParams(vmem_limit_bytes=16 * 2**20),
    )(*arrays)


def plain(
    train_query,
    low_query,
    high_query,
    train_key,
    low_key,
    high_key,
    train_value,
    low_value,
    high_value,
    norm_train,
    norm_step,
):
    def merged(train, low, high):
        update = jnp.dot(low, high, preferred_element_type=jnp.float32)
        fresh = train.astype(jnp.float32) + mix_rate * update
        return lax.all_gather(fresh.astype(jnp.bfloat16), "rows", axis=0, tiled=True).T

    serve_norm = lax.all_gather(
        (norm_train + norm_step).astype(jnp.bfloat16), ("rows", "tp"), axis=0, tiled=True
    )
    return (
        merged(train_query, low_query, high_query),
        merged(train_key, low_key, high_key),
        merged(train_value, low_value, high_value),
        serve_norm,
    )


def solution(mesh):
    size, tp_size = mesh.shape["rows"], mesh.shape["tp"]

    def local(*args):
        trains = (args[0], args[3], args[6])
        fits = (
            size % 2 == 0
            and size >= 4
            and tp_size > 1
            and mesh.shape["job"] > 1
            and SMALL_ROWS % (8 * size) == 0
            and all(t.shape[0] % 128 == 0 and t.shape[1] % CHUNK_ROWS == 0 for t in trains)
            and 2 * trains[0].shape[1] >= sum(t.shape[1] for t in trains)
            and args[9].shape[0] % 128 == 0
        )
        return fused(size, tp_size, *args) if fits else plain(*args)

    in_specs = (
        P(("job", "rows"), "tp"),
        P(("job", "rows"), None),
        P("job", "tp"),
        P(("job", "rows"), "tp"),
        P(("job", "rows"), None),
        P("job", "tp"),
        P(("job", "rows"), "tp"),
        P(("job", "rows"), None),
        P("job", "tp"),
        P(("job", "rows", "tp")),
        P(("job", "rows", "tp")),
    )
    out_specs = (P(("job", "tp"), None), P(("job", "tp"), None), P(("job", "tp"), None), P("job"))
    return jax.shard_map(local, mesh=mesh, in_specs=in_specs, out_specs=out_specs, check_vma=False)
```

```python
import functools

import jax
import jax.numpy as jnp
from jax import lax
from jax.experimental import pallas as pl
from jax.experimental.pallas import tpu as pltpu
from jax.sharding import PartitionSpec as P

mix_rate = 0.5
CHUNK_ROWS = 512
UNIT_ROWS = 256
SMALL_ROWS = 128
RELIEF = 0
VMEM_BYTES = 67043328
MESH = pl.DeviceIdType.MESH


def cuts(length, first):
    sizes = [SMALL_ROWS, CHUNK_ROWS - SMALL_ROWS] if first else []
    length -= sum(sizes)
    while length:
        sizes.append(min(length, CHUNK_ROWS))
        length -= sizes[-1]
    start, found = 0, []
    for rows in sizes:
        found.append((start, rows))
        start += rows
    return found


def units(chunks):
    found = []
    for c, (start, rows) in enumerate(chunks):
        at = start
        while at < start + rows:
            step = SMALL_ROWS if len(found) < 2 else min(UNIT_ROWS, start + rows - at)
            found.append((c, at, step))
            at += step
    return found


def crossed(rows):
    twice, left = [], sum(rows) // 2
    for c in sorted(range(len(rows)), key=lambda c: -rows[c]):
        if c != RELIEF and rows[c] <= left:
            twice.append(c)
            left -= rows[c]
    return sorted(twice)


def kernel(
    size,
    tp_size,
    *refs,
):
    given, refs = refs[:11], refs[11:]
    serve_query, serve_key, serve_value, serve_norm = refs[:4]
    held, refs = refs[4:15], refs[15:]
    run_kernel(size, tp_size, given, held, serve_query, serve_key, serve_value, serve_norm, *refs)


def run_kernel(
    size,
    tp_size,
    given,
    held,
    serve_query,
    serve_key,
    serve_value,
    serve_norm,
    gains,
    send_sem,
    line_sem,
    cross_sem,
    rest_sem,
    gain_send,
    gain_line,
    gain_rest,
    pair_send,
    pair_recv,
    stage,
    stage_sem,
):
    (
        train_query,
        low_query,
        high_query,
        train_key,
        low_key,
        high_key,
        train_value,
        low_value,
        high_value,
        norm_train,
        norm_step,
    ) = held
    depth = size // 2
    me = lax.axis_index("rows")
    core = lax.axis_index("tp")
    z, x = me // 2, lax.rem(me, 2)
    other = 1 - x
    width = train_query.shape[0]
    up, down, side = me + 2, me - 2, 2 * z + other
    targets = (up, down, side)
    has_up, has_down = z < depth - 1, z > 0
    UP, DOWN, SIDE = 0, 1, 2

    def partner(k):
        return {"tp": lax.rem(core + k, tp_size)}

    barrier = pltpu.get_barrier_semaphore()

    def greet(device):
        pl.semaphore_signal(barrier, inc=1, device_id=device, device_id_type=MESH)

    @pl.when(has_up)
    def _():
        greet({"rows": up})

    @pl.when(has_down)
    def _():
        greet({"rows": down})

    greet({"rows": side})
    for k in range(1, tp_size):
        greet(partner(k))
    job = lax.axis_index("job")
    near = (core == 0) & ((me == 1) | (me == 2))
    source, helper = near & (job == 0), near & (job == 1)

    @pl.when((core == 0) & (me == 0) & (job == 0))
    def _():
        for row in (1, 2):
            greet({"job": 1, "rows": row})

    @pl.when(helper)
    def _():
        greet({"job": 0})

    chunks = []
    for train, low, high, serve in (
        (train_query, low_query, high_query, serve_query),
        (train_key, low_key, high_key, serve_key),
        (train_value, low_value, high_value, serve_value),
    ):
        for start, rows in cuts(serve.shape[0], not chunks):
            chunks.append((train, low, high, serve, start, rows))
    count = len(chunks)
    parts = units([c[4:] for c in chunks])
    queries = sum(chunks[c][3] is serve_query for c, _, _ in parts)
    crossings = crossed([c[5] for c in chunks])
    tall = sum(c[5] for c in chunks)
    cross_tall = sum(chunks[c][5] for c in crossings)

    def piece(item, c, part=None):
        if c == count:
            return gains.at[item]
        serve, start, rows = chunks[c][3:]
        if part is not None:
            _, start, rows = part
        return serve.at[pl.ds(start, rows), pl.ds(pl.multiple_of(item * width, 128), width)]

    def landing(item, c, way, own_side):
        slot = item // 2 - 1 if way == DOWN else item // 2
        if c == count:
            return gain_rest.at[0] if way == SIDE else gain_line.at[slot]
        if way != SIDE:
            return line_sem.at[slot, c]
        if own_side and crossing(c):
            return cross_sem.at[crossings.index(c)]
        return rest_sem.at[0]

    def copy(item, c, way, recv, part=None):
        ref = piece(item, c, part)
        return pltpu.make_async_remote_copy(
            src_ref=ref,
            dst_ref=ref,
            send_sem=gain_send.at[0] if c == count else send_sem.at[way],
            recv_sem=recv,
            device_id={"rows": targets[way]},
            device_id_type=MESH,
        )

    def send(item, c, way, own=False, part=None):
        copy(item, c, way, landing(item, c, way, own), part).start()

    def arrive_line(item, c, way):
        copy(item, c, way, landing(item, c, way, False)).wait_recv()

    def bulk(ref, send, recv):
        return pltpu.make_async_remote_copy(
            src_ref=ref,
            dst_ref=ref,
            send_sem=send,
            recv_sem=recv,
            device_id={"rows": side},
            device_id_type=MESH,
        )

    def span(rows):
        return serve_query.at[pl.ds(0, rows // size), :]

    def crossing(c):
        return c in crossings

    def merge(n):
        c, start, length = parts[n]
        train, low, high, serve = chunks[c][:4]
        rows = pl.ds(start, length)
        update = lax.dot_general(
            high[:, rows], low[...], (((0,), (0,)), ((), ())), preferred_element_type=jnp.float32
        )
        fresh = train[:, rows].T.astype(jnp.float32) + mix_rate * update
        serve[rows, pl.ds(pl.multiple_of(me * width, 128), width)] = fresh.astype(jnp.bfloat16)

    def send_own(c, part=None):
        down, across = has_down, True
        if c == RELIEF:
            down, across = has_down & ~(source & (me == 2)), ~(source & (me == 1))

            @pl.when(source)
            def _():
                hand_over().start()

        @pl.when(down)
        def _():
            send(me, c, DOWN, part=part)

        @pl.when(has_up)
        def _():
            send(me, c, UP, part=part)

        @pl.when(across)
        def _():
            send(me, c, SIDE, own=True, part=part)

    def hand_over():
        return pltpu.make_async_remote_copy(
            src_ref=piece(me, RELIEF),
            dst_ref=stage,
            send_sem=stage_sem.at[0],
            recv_sem=stage_sem.at[1],
            device_id={"job": 1},
            device_id_type=MESH,
        )

    def relieve(way):
        return pltpu.make_async_remote_copy(
            src_ref=stage,
            dst_ref=piece(me, RELIEF),
            send_sem=stage_sem.at[0],
            recv_sem=landing(me, RELIEF, way, True),
            device_id={"job": 0, "rows": 0},
            device_id_type=MESH,
        )

    def gain_copy(k):
        return pltpu.make_async_remote_copy(
            src_ref=gains.at[me, core],
            dst_ref=gains.at[me, core],
            send_sem=pair_send.at[k - 1],
            recv_sem=pair_recv.at[k - 1],
            device_id=partner(k),
            device_id_type=MESH,
        )

    def front(load_sem):
        loads = [
            pltpu.make_async_copy(g, h, load_sem.at[n]) for n, (g, h) in enumerate(zip(given, held))
        ]
        for load in loads:
            load.start()
        for n in (0, 1, 2, 9, 10):
            loads[n].wait()
        gains[pl.ds(me, 1), pl.ds(core, 1)] = (norm_train[...] + norm_step[...])[None, None]
        merge(0)
        merge(1)
        expected = sum(e.astype(jnp.int32) for e in (has_up, has_down, source, helper))
        pl.semaphore_wait(barrier, tp_size + expected)
        for n in range(2, len(parts) + 2):
            send_own(parts[n - 2][0], parts[n - 2])
            if n < len(parts):
                if n == queries:
                    for m in range(3, 9):
                        loads[m].wait()
                merge(n)
            if n == 3:
                for k in range(1, tp_size):
                    gain_copy(k).start()

    pl.run_scoped(front, pltpu.SemaphoreType.DMA((len(given),)))
    for k in range(1, tp_size):
        gain_copy(k).wait_recv()
    send_own(count)

    @pl.when(helper)
    def _():
        hand_over().wait_recv()

        @pl.when(me == 1)
        def _():
            relieve(SIDE).start()

        @pl.when(me == 2)
        def _():
            relieve(DOWN).start()

    def pass_on(step, c):
        below, above = me - 2 * step, me + 2 * step

        @pl.when(z >= step)
        def _():
            arrive_line(below, c, UP)

            @pl.when(has_up)
            def _():
                send(below, c, UP)

            if not (step == 1 and crossing(c)):
                send(below, c, SIDE)

        @pl.when(z + step < depth)
        def _():
            arrive_line(above, c, DOWN)

            @pl.when(has_down)
            def _():
                send(above, c, DOWN)

            if not (step == 1 and crossing(c)):
                send(above, c, SIDE)

    def cross(c):
        copy(side, c, SIDE, landing(side, c, SIDE, True)).wait_recv()

        @pl.when(has_down)
        def _():
            copy(side, c, DOWN, rest_sem.at[0]).start()

        @pl.when(has_up)
        def _():
            copy(side, c, UP, rest_sem.at[0]).start()

    order = [c for c in range(count + 1) if c != RELIEF] + [RELIEF]
    for step in range(1, depth):
        for c in order:
            pass_on(step, c)
        if step == max(1, depth - 2):
            for c in crossings:
                cross(c)

    bulk(gains.at[pl.ds(0, depth)], gain_send.at[0], gain_rest.at[0]).wait_recv()
    serve_norm[...] = gains[:size].reshape(serve_norm.shape).astype(jnp.bfloat16)
    bulk(span(depth * tall - cross_tall), send_sem.at[SIDE], rest_sem.at[0]).wait_recv()

    for k in range(1, tp_size):
        gain_copy(k).wait_send()
    @pl.when(source)
    def _():
        hand_over().wait_send()

    @pl.when(helper)
    def _():
        relieve(SIDE).wait_send()

    for level in range(depth):
        has = {UP: level < depth - 1, DOWN: level > 0, SIDE: True}
        rows = {
            UP: (level + 1) * tall + cross_tall,
            DOWN: (depth - level) * tall + cross_tall,
            SIDE: depth * tall - (has[UP] + has[DOWN]) * cross_tall,
        }
        items = {UP: level + 1, DOWN: depth - level, SIDE: depth}
        ways = [way for way in (UP, DOWN, SIDE) if has[way]]

        def drain(less):
            for way in ways:
                sent = span(rows[way] - less.get(way, 0))
                bulk(sent, send_sem.at[way], rest_sem.at[0]).wait_send()

        @pl.when((z == level) & ~source)
        def _():
            drain({})

        if level < 2:

            @pl.when((z == level) & source)
            def _():
                drain({DOWN if level else SIDE: chunks[RELIEF][5]})

        @pl.when(z == level)
        def _():
            sent = gains.at[pl.ds(0, sum(items[way] for way in ways))]
            bulk(sent, gain_send.at[0], gain_rest.at[0]).wait_send()


def fused(size, tp_size, *args):
    train_query, train_key, train_value, norm_train = args[0], args[3], args[6], args[9]
    seats, norm_length = size * tp_size, norm_train.shape[0]
    args = [a.T if n in (1, 4, 7) else a for n, a in enumerate(args)]
    args = [a.reshape(1, -1) if a.ndim == 1 else a for a in args]
    full = train_query.shape[0] * size
    outs = [
        pltpu.VMEM((t.shape[1], full), jnp.bfloat16)
        for t in (train_query, train_key, train_value)
    ]
    outs.append(pltpu.VMEM((seats, norm_length), jnp.bfloat16))
    lengths = [t.shape[1] for t in (train_query, train_key, train_value)]
    sizes = [rows for n, length in enumerate(lengths) for _, rows in cuts(length, n == 0)]
    count = len(sizes)
    grant = VMEM_BYTES - 2 * (sum(t.shape[1] for t in (train_query, train_key, train_value)) * full)
    grant -= 2 * seats * norm_length
    vmem = pl.BlockSpec(memory_space=pltpu.VMEM)
    query, key, value, norm = pl.pallas_call(
        functools.partial(kernel, size, tp_size),
        out_shape=outs,
        in_specs=[pl.BlockSpec(memory_space=pltpu.HBM)] * 11,
        out_specs=[vmem] * 4,
        scratch_shapes=[pltpu.VMEM(a.shape, a.dtype) for a in args]
        + [
            pltpu.VMEM((2 * size, tp_size, 1, norm_length), jnp.float32),
            pltpu.SemaphoreType.DMA((3,)),
            pltpu.SemaphoreType.DMA((size // 2 - 1, count)),
            pltpu.SemaphoreType.DMA((len(crossed(sizes)),)),
            pltpu.SemaphoreType.DMA((1,)),
            pltpu.SemaphoreType.DMA((1,)),
            pltpu.SemaphoreType.DMA((size // 2 - 1,)),
            pltpu.SemaphoreType.DMA((1,)),
            pltpu.SemaphoreType.DMA((tp_size - 1,)),
            pltpu.SemaphoreType.DMA((tp_size - 1,)),
            pltpu.VMEM((SMALL_ROWS, train_query.shape[0]), jnp.bfloat16),
            pltpu.SemaphoreType.DMA((2,)),
        ],
        compiler_params=pltpu.CompilerParams(
            collective_id=0, has_side_effects=True, vmem_limit_bytes=grant
        ),
    )(*args)
    query, key, value, norm = store_out(query, key, value, norm)
    return query, key, value, norm.reshape(-1)


def store_kernel(*refs):
    ins, outs, sems = refs[:4], refs[4:8], refs[8]
    copies = [pltpu.make_async_copy(i, o, sems.at[n]) for n, (i, o) in enumerate(zip(ins, outs))]
    for c in copies:
        c.start()
    for c in copies:
        c.wait()


def store_out(*arrays):
    return pl.pallas_call(
        store_kernel,
        out_shape=[jax.ShapeDtypeStruct(a.shape, a.dtype) for a in arrays],
        in_specs=[pl.BlockSpec(memory_space=pltpu.VMEM)] * 4,
        out_specs=[pl.BlockSpec(memory_space=pltpu.HBM)] * 4,
        scratch_shapes=[pltpu.SemaphoreType.DMA((4,))],
        compiler_params=pltpu.CompilerParams(vmem_limit_bytes=16 * 2**20),
    )(*arrays)


def plain(
    train_query,
    low_query,
    high_query,
    train_key,
    low_key,
    high_key,
    train_value,
    low_value,
    high_value,
    norm_train,
    norm_step,
):
    def merged(train, low, high):
        update = jnp.dot(low, high, preferred_element_type=jnp.float32)
        fresh = train.astype(jnp.float32) + mix_rate * update
        return lax.all_gather(fresh.astype(jnp.bfloat16), "rows", axis=0, tiled=True).T

    serve_norm = lax.all_gather(
        (norm_train + norm_step).astype(jnp.bfloat16), ("rows", "tp"), axis=0, tiled=True
    )
    return (
        merged(train_query, low_query, high_query),
        merged(train_key, low_key, high_key),
        merged(train_value, low_value, high_value),
        serve_norm,
    )


def solution(mesh):
    size, tp_size = mesh.shape["rows"], mesh.shape["tp"]

    def local(*args):
        trains = (args[0], args[3], args[6])
        fits = (
            size % 2 == 0
            and size >= 4
            and tp_size > 1
            and mesh.shape["job"] > 1
            and SMALL_ROWS % (8 * size) == 0
            and all(t.shape[0] % 128 == 0 and t.shape[1] % SMALL_ROWS == 0 for t in trains)
            and trains[0].shape[1] >= 2 * CHUNK_ROWS
            and 2 * trains[0].shape[1] >= sum(t.shape[1] for t in trains)
            and args[9].shape[0] % 128 == 0
        )
        return fused(size, tp_size, *args) if fits else plain(*args)

    in_specs = (
        P(("job", "rows"), "tp"),
        P(("job", "rows"), None),
        P("job", "tp"),
        P(("job", "rows"), "tp"),
        P(("job", "rows"), None),
        P("job", "tp"),
        P(("job", "rows"), "tp"),
        P(("job", "rows"), None),
        P("job", "tp"),
        P(("job", "rows", "tp")),
        P(("job", "rows", "tp")),
    )
    out_specs = (P(("job", "tp"), None), P(("job", "tp"), None), P(("job", "tp"), None), P("job"))
    return jax.shard_map(local, mesh=mesh, in_specs=in_specs, out_specs=out_specs, check_vma=False)
```

```python
import functools

import jax
import jax.numpy as jnp
from jax import lax
from jax.experimental import pallas as pl
from jax.experimental.pallas import tpu as pltpu
from jax.sharding import PartitionSpec as P

mix_rate = 0.5
CHUNK_ROWS = 512
UNIT_ROWS = 256
SMALL_ROWS = 128
RELIEF = 0
LOAD_SEMS = (0, 1, 2, 3, 3, 3, 3, 3, 3, 4, 4)
VMEM_BYTES = 67043328
MESH = pl.DeviceIdType.MESH


def cuts(length, first):
    sizes = [SMALL_ROWS, CHUNK_ROWS - SMALL_ROWS] if first else []
    length -= sum(sizes)
    while length:
        sizes.append(min(length, CHUNK_ROWS))
        length -= sizes[-1]
    start, found = 0, []
    for rows in sizes:
        found.append((start, rows))
        start += rows
    return found


def units(chunks):
    found = []
    for c, (start, rows) in enumerate(chunks):
        at = start
        while at < start + rows:
            step = SMALL_ROWS if len(found) < 2 else min(UNIT_ROWS, start + rows - at)
            found.append((c, at, step))
            at += step
    return found


def crossed(rows):
    twice, left = [], sum(rows) // 2
    for c in sorted(range(len(rows)), key=lambda c: -rows[c]):
        if c != RELIEF and rows[c] <= left:
            twice.append(c)
            left -= rows[c]
    return sorted(twice)


def kernel(
    size,
    tp_size,
    *refs,
):
    given, refs = refs[:11], refs[11:]
    serve_query, serve_key, serve_value, serve_norm = refs[:4]
    held, refs = refs[4:15], refs[15:]
    run_kernel(size, tp_size, given, held, serve_query, serve_key, serve_value, serve_norm, *refs)


def run_kernel(
    size,
    tp_size,
    given,
    held,
    serve_query,
    serve_key,
    serve_value,
    serve_norm,
    gains,
    load_sem,
    send_sem,
    line_sem,
    cross_sem,
    rest_sem,
    gain_send,
    gain_line,
    gain_rest,
    pair_send,
    pair_recv,
    stage,
    stage_sem,
):
    loads = [
        pltpu.make_async_copy(g, h, load_sem.at[LOAD_SEMS[n]])
        for n, (g, h) in enumerate(zip(given, held))
    ]
    (
        train_query,
        low_query,
        high_query,
        train_key,
        low_key,
        high_key,
        train_value,
        low_value,
        high_value,
        norm_train,
        norm_step,
    ) = held
    depth = size // 2
    me = lax.axis_index("rows")
    core = lax.axis_index("tp")
    z, x = me // 2, lax.rem(me, 2)
    other = 1 - x
    width = train_query.shape[0]
    up, down, side = me + 2, me - 2, 2 * z + other
    targets = (up, down, side)
    has_up, has_down = z < depth - 1, z > 0
    UP, DOWN, SIDE = 0, 1, 2

    def partner(k):
        return {"tp": lax.rem(core + k, tp_size)}

    barrier = pltpu.get_barrier_semaphore()

    def greet(device):
        pl.semaphore_signal(barrier, inc=1, device_id=device, device_id_type=MESH)

    @pl.when(has_up)
    def _():
        greet({"rows": up})

    @pl.when(has_down)
    def _():
        greet({"rows": down})

    greet({"rows": side})
    for k in range(1, tp_size):
        greet(partner(k))
    job = lax.axis_index("job")
    near = (core == 0) & ((me == 1) | (me == 2))
    source, helper = near & (job == 0), near & (job == 1)

    @pl.when((core == 0) & (me == 0) & (job == 0))
    def _():
        for row in (1, 2):
            greet({"job": 1, "rows": row})

    @pl.when(helper)
    def _():
        greet({"job": 0})

    for load in loads:
        load.start()

    chunks = []
    for train, low, high, serve in (
        (train_query, low_query, high_query, serve_query),
        (train_key, low_key, high_key, serve_key),
        (train_value, low_value, high_value, serve_value),
    ):
        for start, rows in cuts(serve.shape[0], not chunks):
            chunks.append((train, low, high, serve, start, rows))
    count = len(chunks)
    parts = units([c[4:] for c in chunks])
    queries = sum(chunks[c][3] is serve_query for c, _, _ in parts)
    crossings = crossed([c[5] for c in chunks])
    tall = sum(c[5] for c in chunks)
    cross_tall = sum(chunks[c][5] for c in crossings)

    def piece(item, c, part=None):
        if c == count:
            return gains.at[item]
        serve, start, rows = chunks[c][3:]
        if part is not None:
            _, start, rows = part
        return serve.at[pl.ds(start, rows), pl.ds(pl.multiple_of(item * width, 128), width)]

    def landing(item, c, way, own_side):
        slot = item // 2 - 1 if way == DOWN else item // 2
        if c == count:
            return gain_rest.at[0] if way == SIDE else gain_line.at[slot]
        if way != SIDE:
            return line_sem.at[slot, c]
        if own_side and crossing(c):
            return cross_sem.at[crossings.index(c)]
        return rest_sem.at[0]

    def copy(item, c, way, recv, part=None):
        ref = piece(item, c, part)
        return pltpu.make_async_remote_copy(
            src_ref=ref,
            dst_ref=ref,
            send_sem=gain_send.at[0] if c == count else send_sem.at[way],
            recv_sem=recv,
            device_id={"rows": targets[way]},
            device_id_type=MESH,
        )

    def send(item, c, way, own=False, part=None):
        copy(item, c, way, landing(item, c, way, own), part).start()

    def arrive_line(item, c, way):
        copy(item, c, way, landing(item, c, way, False)).wait_recv()

    def bulk(ref, send, recv):
        return pltpu.make_async_remote_copy(
            src_ref=ref,
            dst_ref=ref,
            send_sem=send,
            recv_sem=recv,
            device_id={"rows": side},
            device_id_type=MESH,
        )

    def span(rows):
        return serve_query.at[pl.ds(0, rows // size), :]

    def crossing(c):
        return c in crossings

    def merge(n):
        c, start, length = parts[n]
        train, low, high, serve = chunks[c][:4]
        rows = pl.ds(start, length)
        update = lax.dot_general(
            high[:, rows], low[...], (((0,), (0,)), ((), ())), preferred_element_type=jnp.float32
        )
        fresh = train[:, rows].T.astype(jnp.float32) + mix_rate * update
        serve[rows, pl.ds(pl.multiple_of(me * width, 128), width)] = fresh.astype(jnp.bfloat16)

    def send_own(c, part=None):
        down, across = has_down, True
        if c == RELIEF:
            down, across = has_down & ~(source & (me == 2)), ~(source & (me == 1))

            @pl.when(source)
            def _():
                hand_over().start()

        @pl.when(down)
        def _():
            send(me, c, DOWN, part=part)

        @pl.when(has_up)
        def _():
            send(me, c, UP, part=part)

        @pl.when(across)
        def _():
            send(me, c, SIDE, own=True, part=part)

    def hand_over():
        return pltpu.make_async_remote_copy(
            src_ref=piece(me, RELIEF),
            dst_ref=stage,
            send_sem=stage_sem.at[0],
            recv_sem=stage_sem.at[1],
            device_id={"job": 1},
            device_id_type=MESH,
        )

    def relieve(way):
        return pltpu.make_async_remote_copy(
            src_ref=stage,
            dst_ref=piece(me, RELIEF),
            send_sem=stage_sem.at[0],
            recv_sem=landing(me, RELIEF, way, True),
            device_id={"job": 0, "rows": 0},
            device_id_type=MESH,
        )

    def gain_copy(k):
        return pltpu.make_async_remote_copy(
            src_ref=gains.at[me, core],
            dst_ref=gains.at[me, core],
            send_sem=pair_send.at[k - 1],
            recv_sem=pair_recv.at[k - 1],
            device_id=partner(k),
            device_id_type=MESH,
        )

    for n in (0, 1, 2):
        loads[n].wait()
    bulk(gains.at[0], pair_send.at[0], load_sem.at[4]).wait_recv()
    gains[pl.ds(me, 1), pl.ds(core, 1)] = (norm_train[...] + norm_step[...])[None, None]
    merge(0)
    merge(1)
    expected = sum(e.astype(jnp.int32) for e in (has_up, has_down, source, helper))
    pl.semaphore_wait(barrier, tp_size + expected)
    for n in range(2, len(parts) + 2):
        send_own(parts[n - 2][0], parts[n - 2])
        if n < len(parts):
            if n == queries:
                loaded = sum(h.shape[0] * h.shape[1] for h in held[3:9]) // (size * width)
                whole = serve_query.at[pl.ds(0, loaded), :]
                bulk(whole, pair_send.at[0], load_sem.at[3]).wait_recv()
            merge(n)
        if n == 3:
            for k in range(1, tp_size):
                gain_copy(k).start()
    for k in range(1, tp_size):
        gain_copy(k).wait_recv()
    send_own(count)

    @pl.when(helper)
    def _():
        hand_over().wait_recv()

        @pl.when(me == 1)
        def _():
            relieve(SIDE).start()

        @pl.when(me == 2)
        def _():
            relieve(DOWN).start()

    def pass_on(step, c):
        below, above = me - 2 * step, me + 2 * step

        @pl.when(z >= step)
        def _():
            arrive_line(below, c, UP)

            @pl.when(has_up)
            def _():
                send(below, c, UP)

            if not (step == 1 and crossing(c)):
                send(below, c, SIDE)

        @pl.when(z + step < depth)
        def _():
            arrive_line(above, c, DOWN)

            @pl.when(has_down)
            def _():
                send(above, c, DOWN)

            if not (step == 1 and crossing(c)):
                send(above, c, SIDE)

    def cross(c):
        copy(side, c, SIDE, landing(side, c, SIDE, True)).wait_recv()

        @pl.when(has_down)
        def _():
            copy(side, c, DOWN, rest_sem.at[0]).start()

        @pl.when(has_up)
        def _():
            copy(side, c, UP, rest_sem.at[0]).start()

    order = [c for c in range(count + 1) if c != RELIEF] + [RELIEF]
    for step in range(1, depth):
        for c in order:
            pass_on(step, c)
        if step == max(1, depth - 2):
            for c in crossings:
                cross(c)

    bulk(gains.at[pl.ds(0, depth)], gain_send.at[0], gain_rest.at[0]).wait_recv()
    serve_norm[...] = gains[:size].reshape(serve_norm.shape).astype(jnp.bfloat16)
    bulk(span(depth * tall - cross_tall), send_sem.at[SIDE], rest_sem.at[0]).wait_recv()

    for k in range(1, tp_size):
        gain_copy(k).wait_send()
    @pl.when(source)
    def _():
        hand_over().wait_send()

    @pl.when(helper)
    def _():
        relieve(SIDE).wait_send()

    for level in range(depth):
        has = {UP: level < depth - 1, DOWN: level > 0, SIDE: True}
        rows = {
            UP: (level + 1) * tall + cross_tall,
            DOWN: (depth - level) * tall + cross_tall,
            SIDE: depth * tall - (has[UP] + has[DOWN]) * cross_tall,
        }
        items = {UP: level + 1, DOWN: depth - level, SIDE: depth}
        ways = [way for way in (UP, DOWN, SIDE) if has[way]]

        def drain(less):
            for way in ways:
                sent = span(rows[way] - less.get(way, 0))
                bulk(sent, send_sem.at[way], rest_sem.at[0]).wait_send()

        @pl.when((z == level) & ~source)
        def _():
            drain({})

        if level < 2:

            @pl.when((z == level) & source)
            def _():
                drain({DOWN if level else SIDE: chunks[RELIEF][5]})

        @pl.when(z == level)
        def _():
            sent = gains.at[pl.ds(0, sum(items[way] for way in ways))]
            bulk(sent, gain_send.at[0], gain_rest.at[0]).wait_send()


def fused(size, tp_size, *args):
    train_query, train_key, train_value, norm_train = args[0], args[3], args[6], args[9]
    seats, norm_length = size * tp_size, norm_train.shape[0]
    args = [a.T if n in (1, 4, 7) else a for n, a in enumerate(args)]
    args = [a.reshape(1, -1) if a.ndim == 1 else a for a in args]
    full = train_query.shape[0] * size
    outs = [
        pltpu.VMEM((t.shape[1], full), jnp.bfloat16)
        for t in (train_query, train_key, train_value)
    ]
    outs.append(pltpu.VMEM((seats, norm_length), jnp.bfloat16))
    lengths = [t.shape[1] for t in (train_query, train_key, train_value)]
    sizes = [rows for n, length in enumerate(lengths) for _, rows in cuts(length, n == 0)]
    count = len(sizes)
    grant = VMEM_BYTES - 2 * (sum(t.shape[1] for t in (train_query, train_key, train_value)) * full)
    grant -= 2 * seats * norm_length
    vmem = pl.BlockSpec(memory_space=pltpu.VMEM)
    query, key, value, norm = pl.pallas_call(
        functools.partial(kernel, size, tp_size),
        out_shape=outs,
        in_specs=[pl.BlockSpec(memory_space=pltpu.HBM)] * 11,
        out_specs=[vmem] * 4,
        scratch_shapes=[pltpu.VMEM(a.shape, a.dtype) for a in args]
        + [
            pltpu.VMEM((2 * size, tp_size, 1, norm_length), jnp.float32),
            pltpu.SemaphoreType.DMA((max(LOAD_SEMS) + 1,)),
            pltpu.SemaphoreType.DMA((3,)),
            pltpu.SemaphoreType.DMA((size // 2 - 1, count)),
            pltpu.SemaphoreType.DMA((len(crossed(sizes)),)),
            pltpu.SemaphoreType.DMA((1,)),
            pltpu.SemaphoreType.DMA((1,)),
            pltpu.SemaphoreType.DMA((size // 2 - 1,)),
            pltpu.SemaphoreType.DMA((1,)),
            pltpu.SemaphoreType.DMA((tp_size - 1,)),
            pltpu.SemaphoreType.DMA((tp_size - 1,)),
            pltpu.VMEM((SMALL_ROWS, train_query.shape[0]), jnp.bfloat16),
            pltpu.SemaphoreType.DMA((2,)),
        ],
        compiler_params=pltpu.CompilerParams(
            collective_id=0, has_side_effects=True, vmem_limit_bytes=grant
        ),
    )(*args)
    query, key, value, norm = store_out(query, key, value, norm)
    return query, key, value, norm.reshape(-1)


def store_kernel(*refs):
    ins, outs, sems = refs[:4], refs[4:8], refs[8]
    copies = [pltpu.make_async_copy(i, o, sems.at[n]) for n, (i, o) in enumerate(zip(ins, outs))]
    for c in copies:
        c.start()
    for c in copies:
        c.wait()


def store_out(*arrays):
    return pl.pallas_call(
        store_kernel,
        out_shape=[jax.ShapeDtypeStruct(a.shape, a.dtype) for a in arrays],
        in_specs=[pl.BlockSpec(memory_space=pltpu.VMEM)] * 4,
        out_specs=[pl.BlockSpec(memory_space=pltpu.HBM)] * 4,
        scratch_shapes=[pltpu.SemaphoreType.DMA((4,))],
        compiler_params=pltpu.CompilerParams(vmem_limit_bytes=16 * 2**20),
    )(*arrays)


def plain(
    train_query,
    low_query,
    high_query,
    train_key,
    low_key,
    high_key,
    train_value,
    low_value,
    high_value,
    norm_train,
    norm_step,
):
    def merged(train, low, high):
        update = jnp.dot(low, high, preferred_element_type=jnp.float32)
        fresh = train.astype(jnp.float32) + mix_rate * update
        return lax.all_gather(fresh.astype(jnp.bfloat16), "rows", axis=0, tiled=True).T

    serve_norm = lax.all_gather(
        (norm_train + norm_step).astype(jnp.bfloat16), ("rows", "tp"), axis=0, tiled=True
    )
    return (
        merged(train_query, low_query, high_query),
        merged(train_key, low_key, high_key),
        merged(train_value, low_value, high_value),
        serve_norm,
    )


def solution(mesh):
    size, tp_size = mesh.shape["rows"], mesh.shape["tp"]

    def local(*args):
        trains = (args[0], args[3], args[6])
        fits = (
            size % 2 == 0
            and size >= 4
            and tp_size == 2
            and mesh.shape["job"] > 1
            and SMALL_ROWS % (8 * size) == 0
            and all(t.shape[0] % 128 == 0 and t.shape[1] % SMALL_ROWS == 0 for t in trains)
            and trains[0].shape[1] >= 2 * CHUNK_ROWS
            and 2 * trains[0].shape[1] >= sum(t.shape[1] for t in trains)
            and args[9].shape[0] % 128 == 0
            and sum(a.size for a in args[3:9]) % (8 * size * trains[0].shape[0]) == 0
        )
        return fused(size, tp_size, *args) if fits else plain(*args)

    in_specs = (
        P(("job", "rows"), "tp"),
        P(("job", "rows"), None),
        P("job", "tp"),
        P(("job", "rows"), "tp"),
        P(("job", "rows"), None),
        P("job", "tp"),
        P(("job", "rows"), "tp"),
        P(("job", "rows"), None),
        P("job", "tp"),
        P(("job", "rows", "tp")),
        P(("job", "rows", "tp")),
    )
    out_specs = (P(("job", "tp"), None), P(("job", "tp"), None), P(("job", "tp"), None), P("job"))
    return jax.shard_map(local, mesh=mesh, in_specs=in_specs, out_specs=out_specs, check_vma=False)
```

```python
import functools

import jax
import jax.numpy as jnp
from jax import lax
from jax.experimental import pallas as pl
from jax.experimental.pallas import tpu as pltpu
from jax.sharding import PartitionSpec as P

mix_rate = 0.5
CHUNK_ROWS = 512
UNIT_ROWS = 256
SMALL_ROWS = 128
RELIEF = 0
LOAD_SEMS = (0, 0, 0, 1, 1, 1, 1, 1, 1, 2, 2)
VMEM_BYTES = 67043328
MESH = pl.DeviceIdType.MESH


def cuts(length, first):
    sizes = [SMALL_ROWS, CHUNK_ROWS - SMALL_ROWS] if first else []
    length -= sum(sizes)
    while length:
        sizes.append(min(length, CHUNK_ROWS))
        length -= sizes[-1]
    start, found = 0, []
    for rows in sizes:
        found.append((start, rows))
        start += rows
    return found


def units(chunks):
    found = []
    for c, (start, rows) in enumerate(chunks):
        at = start
        while at < start + rows:
            step = SMALL_ROWS if len(found) < 2 else min(UNIT_ROWS, start + rows - at)
            found.append((c, at, step))
            at += step
    return found


def crossed(rows):
    twice, left = [], sum(rows) // 2
    for c in sorted(range(len(rows)), key=lambda c: -rows[c]):
        if c != RELIEF and rows[c] <= left:
            twice.append(c)
            left -= rows[c]
    return sorted(twice)


def kernel(
    size,
    tp_size,
    *refs,
):
    given, refs = refs[:11], refs[11:]
    serve_query, serve_key, serve_value, serve_norm = refs[:4]
    held, refs = refs[4:15], refs[15:]
    run_kernel(size, tp_size, given, held, serve_query, serve_key, serve_value, serve_norm, *refs)


def run_kernel(
    size,
    tp_size,
    given,
    held,
    serve_query,
    serve_key,
    serve_value,
    serve_norm,
    gains,
    load_sem,
    send_sem,
    line_sem,
    cross_sem,
    rest_sem,
    gain_send,
    gain_line,
    gain_rest,
    pair_send,
    pair_recv,
    stage,
    stage_sem,
):
    loads = [
        pltpu.make_async_copy(g, h, load_sem.at[LOAD_SEMS[n]])
        for n, (g, h) in enumerate(zip(given, held))
    ]
    (
        train_query,
        low_query,
        high_query,
        train_key,
        low_key,
        high_key,
        train_value,
        low_value,
        high_value,
        norm_train,
        norm_step,
    ) = held
    depth = size // 2
    me = lax.axis_index("rows")
    core = lax.axis_index("tp")
    z, x = me // 2, lax.rem(me, 2)
    other = 1 - x
    width = train_query.shape[0]
    up, down, side = me + 2, me - 2, 2 * z + other
    targets = (up, down, side)
    has_up, has_down = z < depth - 1, z > 0
    UP, DOWN, SIDE = 0, 1, 2

    def partner(k):
        return {"tp": lax.rem(core + k, tp_size)}

    barrier = pltpu.get_barrier_semaphore()

    def greet(device):
        pl.semaphore_signal(barrier, inc=1, device_id=device, device_id_type=MESH)

    @pl.when(has_up)
    def _():
        greet({"rows": up})

    @pl.when(has_down)
    def _():
        greet({"rows": down})

    greet({"rows": side})
    for k in range(1, tp_size):
        greet(partner(k))
    job = lax.axis_index("job")
    near = (core == 0) & ((me == 1) | (me == 2))
    source, helper = near & (job == 0), near & (job == 1)

    @pl.when((core == 0) & (me == 0) & (job == 0))
    def _():
        for row in (1, 2):
            greet({"job": 1, "rows": row})

    @pl.when(helper)
    def _():
        greet({"job": 0})

    for load in loads:
        load.start()

    chunks = []
    for train, low, high, serve in (
        (train_query, low_query, high_query, serve_query),
        (train_key, low_key, high_key, serve_key),
        (train_value, low_value, high_value, serve_value),
    ):
        for start, rows in cuts(serve.shape[0], not chunks):
            chunks.append((train, low, high, serve, start, rows))
    count = len(chunks)
    parts = units([c[4:] for c in chunks])
    queries = sum(chunks[c][3] is serve_query for c, _, _ in parts)
    crossings = crossed([c[5] for c in chunks])
    tall = sum(c[5] for c in chunks)
    cross_tall = sum(chunks[c][5] for c in crossings)

    def piece(item, c, part=None):
        if c == count:
            return gains.at[item]
        serve, start, rows = chunks[c][3:]
        if part is not None:
            _, start, rows = part
        return serve.at[pl.ds(start, rows), pl.ds(pl.multiple_of(item * width, 128), width)]

    def landing(item, c, way, own_side):
        slot = item // 2 - 1 if way == DOWN else item // 2
        if c == count:
            return gain_rest.at[0] if way == SIDE else gain_line.at[slot]
        if way != SIDE:
            return line_sem.at[slot, c]
        if own_side and crossing(c):
            return cross_sem.at[0]
        return rest_sem.at[0]

    def copy(item, c, way, recv, part=None):
        ref = piece(item, c, part)
        return pltpu.make_async_remote_copy(
            src_ref=ref,
            dst_ref=ref,
            send_sem=gain_send.at[0] if c == count else send_sem.at[way],
            recv_sem=recv,
            device_id={"rows": targets[way]},
            device_id_type=MESH,
        )

    def send(item, c, way, own=False, part=None):
        copy(item, c, way, landing(item, c, way, own), part).start()

    def arrive_line(item, c, way):
        copy(item, c, way, landing(item, c, way, False)).wait_recv()

    def bulk(ref, send, recv):
        return pltpu.make_async_remote_copy(
            src_ref=ref,
            dst_ref=ref,
            send_sem=send,
            recv_sem=recv,
            device_id={"rows": side},
            device_id_type=MESH,
        )

    def span(rows):
        return serve_query.at[pl.ds(0, rows // size), :]

    def crossing(c):
        return c in crossings

    def merge(n):
        c, start, length = parts[n]
        train, low, high, serve = chunks[c][:4]
        rows = pl.ds(start, length)
        update = lax.dot_general(
            high[:, rows], low[...], (((0,), (0,)), ((), ())), preferred_element_type=jnp.float32
        )
        fresh = train[:, rows].T.astype(jnp.float32) + mix_rate * update
        serve[rows, pl.ds(pl.multiple_of(me * width, 128), width)] = fresh.astype(jnp.bfloat16)

    def send_own(c, part=None):
        down, across = has_down, True
        if c == RELIEF:
            down, across = has_down & ~(source & (me == 2)), ~(source & (me == 1))

            @pl.when(source)
            def _():
                hand_over().start()

        @pl.when(down)
        def _():
            send(me, c, DOWN, part=part)

        @pl.when(has_up)
        def _():
            send(me, c, UP, part=part)

        @pl.when(across)
        def _():
            send(me, c, SIDE, own=True, part=part)

    def hand_over():
        return pltpu.make_async_remote_copy(
            src_ref=piece(me, RELIEF),
            dst_ref=stage,
            send_sem=stage_sem.at[0],
            recv_sem=stage_sem.at[1],
            device_id={"job": 1},
            device_id_type=MESH,
        )

    def relieve(way):
        return pltpu.make_async_remote_copy(
            src_ref=stage,
            dst_ref=piece(me, RELIEF),
            send_sem=stage_sem.at[0],
            recv_sem=landing(me, RELIEF, way, True),
            device_id={"job": 0, "rows": 0},
            device_id_type=MESH,
        )

    def gain_copy(k):
        return pltpu.make_async_remote_copy(
            src_ref=gains.at[me, core],
            dst_ref=gains.at[me, core],
            send_sem=pair_send.at[k - 1],
            recv_sem=pair_recv.at[k - 1],
            device_id=partner(k),
            device_id_type=MESH,
        )

    loaded = sum(h.shape[0] * h.shape[1] for h in held[:3]) // (2 * width)
    block = serve_query.at[pl.ds(0, loaded), pl.ds(0, 2 * width)]
    bulk(block, pair_send.at[0], load_sem.at[0]).wait_recv()
    bulk(gains.at[0], pair_send.at[0], load_sem.at[2]).wait_recv()
    gains[pl.ds(me, 1), pl.ds(core, 1)] = (norm_train[...] + norm_step[...])[None, None]
    merge(0)
    merge(1)
    expected = sum(e.astype(jnp.int32) for e in (has_up, has_down, source, helper))
    pl.semaphore_wait(barrier, tp_size + expected)
    for n in range(2, len(parts) + 2):
        send_own(parts[n - 2][0], parts[n - 2])
        if n < len(parts):
            if n == queries:
                loaded = sum(h.shape[0] * h.shape[1] for h in held[3:9]) // (size * width)
                whole = serve_query.at[pl.ds(0, loaded), :]
                bulk(whole, pair_send.at[0], load_sem.at[1]).wait_recv()
            merge(n)
        if n == 3:
            for k in range(1, tp_size):
                gain_copy(k).start()
    for k in range(1, tp_size):
        gain_copy(k).wait_recv()
    send_own(count)

    @pl.when(helper)
    def _():
        hand_over().wait_recv()

        @pl.when(me == 1)
        def _():
            relieve(SIDE).start()

        @pl.when(me == 2)
        def _():
            relieve(DOWN).start()

    def pass_on(step, c):
        below, above = me - 2 * step, me + 2 * step

        @pl.when(z >= step)
        def _():
            arrive_line(below, c, UP)

            @pl.when(has_up)
            def _():
                send(below, c, UP)

            if not (step == 1 and crossing(c)):
                send(below, c, SIDE)

        @pl.when(z + step < depth)
        def _():
            arrive_line(above, c, DOWN)

            @pl.when(has_down)
            def _():
                send(above, c, DOWN)

            if not (step == 1 and crossing(c)):
                send(above, c, SIDE)

    def cross(c):
        @pl.when(has_down)
        def _():
            copy(side, c, DOWN, rest_sem.at[0]).start()

        @pl.when(has_up)
        def _():
            copy(side, c, UP, rest_sem.at[0]).start()

    order = [c for c in range(count + 1) if c != RELIEF] + [RELIEF]
    for step in range(1, depth):
        for c in order:
            pass_on(step, c)
        if step == max(1, depth - 2):
            bulk(span(cross_tall), send_sem.at[SIDE], cross_sem.at[0]).wait_recv()
            for c in crossings:
                cross(c)

    bulk(gains.at[pl.ds(0, depth)], gain_send.at[0], gain_rest.at[0]).wait_recv()
    serve_norm[...] = gains[:size].reshape(serve_norm.shape).astype(jnp.bfloat16)
    bulk(span(depth * tall - cross_tall), send_sem.at[SIDE], rest_sem.at[0]).wait_recv()

    for k in range(1, tp_size):
        gain_copy(k).wait_send()
    @pl.when(source)
    def _():
        hand_over().wait_send()

    @pl.when(helper)
    def _():
        relieve(SIDE).wait_send()

    for level in range(depth):
        has = {UP: level < depth - 1, DOWN: level > 0, SIDE: True}
        rows = {
            UP: (level + 1) * tall + cross_tall,
            DOWN: (depth - level) * tall + cross_tall,
            SIDE: depth * tall - (has[UP] + has[DOWN]) * cross_tall,
        }
        items = {UP: level + 1, DOWN: depth - level, SIDE: depth}
        ways = [way for way in (UP, DOWN, SIDE) if has[way]]

        def drain(less):
            for way in ways:
                sent = span(rows[way] - less.get(way, 0))
                bulk(sent, send_sem.at[way], rest_sem.at[0]).wait_send()

        @pl.when((z == level) & ~source)
        def _():
            drain({})

        if level < 2:

            @pl.when((z == level) & source)
            def _():
                drain({DOWN if level else SIDE: chunks[RELIEF][5]})

        @pl.when(z == level)
        def _():
            sent = gains.at[pl.ds(0, sum(items[way] for way in ways))]
            bulk(sent, gain_send.at[0], gain_rest.at[0]).wait_send()


def fused(size, tp_size, *args):
    train_query, train_key, train_value, norm_train = args[0], args[3], args[6], args[9]
    seats, norm_length = size * tp_size, norm_train.shape[0]
    args = [a.T if n in (1, 4, 7) else a for n, a in enumerate(args)]
    args = [a.reshape(1, -1) if a.ndim == 1 else a for a in args]
    full = train_query.shape[0] * size
    outs = [
        pltpu.VMEM((t.shape[1], full), jnp.bfloat16)
        for t in (train_query, train_key, train_value)
    ]
    outs.append(pltpu.VMEM((seats, norm_length), jnp.bfloat16))
    lengths = [t.shape[1] for t in (train_query, train_key, train_value)]
    sizes = [rows for n, length in enumerate(lengths) for _, rows in cuts(length, n == 0)]
    count = len(sizes)
    grant = VMEM_BYTES - 2 * (sum(t.shape[1] for t in (train_query, train_key, train_value)) * full)
    grant -= 2 * seats * norm_length
    vmem = pl.BlockSpec(memory_space=pltpu.VMEM)
    query, key, value, norm = pl.pallas_call(
        functools.partial(kernel, size, tp_size),
        out_shape=outs,
        in_specs=[pl.BlockSpec(memory_space=pltpu.HBM)] * 11,
        out_specs=[vmem] * 4,
        scratch_shapes=[pltpu.VMEM(a.shape, a.dtype) for a in args]
        + [
            pltpu.VMEM((2 * size, tp_size, 1, norm_length), jnp.float32),
            pltpu.SemaphoreType.DMA((max(LOAD_SEMS) + 1,)),
            pltpu.SemaphoreType.DMA((3,)),
            pltpu.SemaphoreType.DMA((size // 2 - 1, count)),
            pltpu.SemaphoreType.DMA((1,)),
            pltpu.SemaphoreType.DMA((1,)),
            pltpu.SemaphoreType.DMA((1,)),
            pltpu.SemaphoreType.DMA((size // 2 - 1,)),
            pltpu.SemaphoreType.DMA((1,)),
            pltpu.SemaphoreType.DMA((tp_size - 1,)),
            pltpu.SemaphoreType.DMA((tp_size - 1,)),
            pltpu.VMEM((SMALL_ROWS, train_query.shape[0]), jnp.bfloat16),
            pltpu.SemaphoreType.DMA((2,)),
        ],
        compiler_params=pltpu.CompilerParams(
            collective_id=0, has_side_effects=True, vmem_limit_bytes=grant
        ),
    )(*args)
    query, key, value, norm = store_out(query, key, value, norm)
    return query, key, value, norm.reshape(-1)


def store_kernel(*refs):
    ins, outs, sems = refs[:4], refs[4:8], refs[8]
    copies = [pltpu.make_async_copy(i, o, sems.at[n]) for n, (i, o) in enumerate(zip(ins, outs))]
    for c in copies:
        c.start()
    for c in copies:
        c.wait()


def store_out(*arrays):
    return pl.pallas_call(
        store_kernel,
        out_shape=[jax.ShapeDtypeStruct(a.shape, a.dtype) for a in arrays],
        in_specs=[pl.BlockSpec(memory_space=pltpu.VMEM)] * 4,
        out_specs=[pl.BlockSpec(memory_space=pltpu.HBM)] * 4,
        scratch_shapes=[pltpu.SemaphoreType.DMA((4,))],
        compiler_params=pltpu.CompilerParams(vmem_limit_bytes=16 * 2**20),
    )(*arrays)


def plain(
    train_query,
    low_query,
    high_query,
    train_key,
    low_key,
    high_key,
    train_value,
    low_value,
    high_value,
    norm_train,
    norm_step,
):
    def merged(train, low, high):
        update = jnp.dot(low, high, preferred_element_type=jnp.float32)
        fresh = train.astype(jnp.float32) + mix_rate * update
        return lax.all_gather(fresh.astype(jnp.bfloat16), "rows", axis=0, tiled=True).T

    serve_norm = lax.all_gather(
        (norm_train + norm_step).astype(jnp.bfloat16), ("rows", "tp"), axis=0, tiled=True
    )
    return (
        merged(train_query, low_query, high_query),
        merged(train_key, low_key, high_key),
        merged(train_value, low_value, high_value),
        serve_norm,
    )


def solution(mesh):
    size, tp_size = mesh.shape["rows"], mesh.shape["tp"]

    def local(*args):
        trains = (args[0], args[3], args[6])
        fits = (
            size % 2 == 0
            and size >= 4
            and tp_size == 2
            and mesh.shape["job"] > 1
            and SMALL_ROWS % (8 * size) == 0
            and all(t.shape[0] % 128 == 0 and t.shape[1] % SMALL_ROWS == 0 for t in trains)
            and trains[0].shape[1] >= 2 * CHUNK_ROWS
            and 2 * trains[0].shape[1] >= sum(t.shape[1] for t in trains)
            and args[9].shape[0] % 128 == 0
            and sum(a.size for a in args[:3]) % (16 * trains[0].shape[0]) == 0
            and sum(a.size for a in args[:3]) <= 2 * trains[0].size
            and sum(a.size for a in args[3:9]) % (8 * size * trains[0].shape[0]) == 0
        )
        return fused(size, tp_size, *args) if fits else plain(*args)

    in_specs = (
        P(("job", "rows"), "tp"),
        P(("job", "rows"), None),
        P("job", "tp"),
        P(("job", "rows"), "tp"),
        P(("job", "rows"), None),
        P("job", "tp"),
        P(("job", "rows"), "tp"),
        P(("job", "rows"), None),
        P("job", "tp"),
        P(("job", "rows", "tp")),
        P(("job", "rows", "tp")),
    )
    out_specs = (P(("job", "tp"), None), P(("job", "tp"), None), P(("job", "tp"), None), P("job"))
    return jax.shard_map(local, mesh=mesh, in_specs=in_specs, out_specs=out_specs, check_vma=False)
```
